256 devices in a mesh: grp: 2 (over core), seq: 16 (over z, x_lo), head: 8 (over x_hi, y).
Axes of the slice: x: 4 (x_hi: 2, x_lo: 2; x = x_hi * 2 + x_lo), y: 4, z: 8, core: 2. Of those that a mesh axis runs over, the one named last changes fastest.
Arguments:
- patches: bfloat16 [4096, 1152], P(('grp', 'seq'), 'head'), may hold values from -200 to 200
- frames: int32 [4096], replicated, may hold values from 0 to 63, never falling along the last dimension, each value on 1 to 128 neighbouring positions
- enc_qkv: bfloat16 [3, 1152, 1152], P(None, None, 'head'), may hold values from -0.1875 to 0.1875
- enc_out: bfloat16 [1152, 1152], P('head'), may hold values from -0.1875 to 0.1875
- merge_gain: float32 [2, 4608], replicated, may hold values from 0.5 to 1.5
- merge_w: bfloat16 [2, 4608, 5120], P(None, ('grp', 'seq'), 'head'), may hold values from -0.09375 to 0.09375
- embedded: bfloat16 [8192, 5120], P(('grp', 'seq'), 'head'), may hold values from -200 to 200
- source: int32 [8192], P(('grp', 'seq')), may hold values from -1 to 1023, as said below
- dec_q: bfloat16 [5120, 4096], P(('grp', 'seq'), 'head'), may hold values from -0.078125 to 0.078125
- dec_kv: bfloat16 [5120, 2048], P(('grp', 'seq'), 'head'), may hold values from -0.078125 to 0.078125
- cotangent: bfloat16 [8192, 2, 5120], P(('grp', 'seq'), None, 'head'), may hold values from -6 to 6
Outputs:
- merged: bfloat16 [2, 1024, 5120], P(None, ('grp', 'seq'), 'head')
- context: bfloat16 [8192, 4096], P(('grp', 'seq'), 'head')
- level_grads: float32 [2, 1024, 5120], P(None, ('grp', 'seq'), 'head')
The draws below stay inside these ranges and needn't reach their ends.
Inputs may be any that keep to these rules, and one draw needn't show every extreme that they name: `frames`: frame numbers never fall along the patches and no frame holds more than 128 patches. `source`: every merged token 0 to 1023 stands at exactly one position; all other positions hold -1; the rows of one device hold exactly 32 merged tokens, and at most 4 of those in one aligned block of 32 merged tokens, a most that some device reaches in every draw.
All inputs are finite; a program needn't handle non-finite values.
Results may differ from the reference program's by a relative error of at most 0.03.
The reference program's roundings to bfloat16 on the way (of `enc_attn`, `enc_hidden`, `normed` and `states`) count: a program that leaves them out, or rounds other values in their place, can miss the bound.
Values may be sent and summed in bfloat16 or wider, within the bound.
No kernel may reach another device: no remote copies, remote signals or barrier semaphores. Data moves between devices by JAX's collectives and lax.ppermute only.
A program may use at most 128 MiB of HBM per device.

```python
import math
import jax
import jax.numpy as jnp
import numpy as np
from jax import lax

ENC_WIDTH = 1152
ENC_HEADS = 16
WIDTH = 5120
Q_HEADS = 32
KV_HEADS = 8
HEAD_DIM = 128
RETURN_MOST = 4
PAT_DEV = 128
TOK_DEV = 256
PATCHES = 4096
MERGED = 1024
TOKENS = 8192


def scaled_rows(key, rows, cols):
    base = jnp.clip(jax.random.normal(key, (rows, cols), jnp.float32), -6.0, 6.0)
    return base.astype(jnp.bfloat16)


def draw_patches(key, part):
    return scaled_rows(jax.random.fold_in(key, 11), PATCHES, ENC_WIDTH)


def draw_embedded(key, part):
    return scaled_rows(jax.random.fold_in(key, 13), TOKENS, WIDTH)


def draw_source(key, part):
    holders = PATCHES // PAT_DEV
    block = PAT_DEV // 4
    runs = block // RETURN_MOST
    half_way = holders // 2
    rest = jax.random.permutation(jax.random.fold_in(key, 17), holders - 2).astype(jnp.int32)
    rest = rest + (rest >= 1).astype(jnp.int32)
    rest = rest + (rest >= half_way).astype(jnp.int32)
    offsets = jnp.concatenate([jnp.array([1, half_way], jnp.int32), rest])[:runs]
    tokens_all = jnp.arange(MERGED, dtype=jnp.int32)
    holder_of = tokens_all // block
    within = tokens_all % block
    device = (holder_of + offsets[within // RETURN_MOST]) % holders
    device_keys = jax.random.split(jax.random.fold_in(key, 19), holders)
    slot_table = jax.vmap(lambda sub: jax.random.permutation(sub, TOK_DEV).astype(jnp.int32))(device_keys)
    position = device * TOK_DEV + slot_table[device, within]
    empty = jnp.full((TOKENS,), -1, jnp.int32)
    return empty.at[position].set(tokens_all)


def steps_of(key, shape, cuts, smallest, high):
    def one(dim, shards_of):
        draws = jax.random.uniform(jax.random.fold_in(jax.random.fold_in(key, 6), dim), (shards_of,), jnp.float32, smallest / len(cuts), high / len(cuts))
        return jnp.repeat(jnp.exp(draws), shape[dim] // shards_of).reshape((-1,) + (1,) * (len(shape) - dim - 1))

    level = one(*cuts[0])
    for cut in cuts[1:]:
        level = level * one(*cut)
    return level


def length_profile(number_of, total, most, skew):
    portions = [(1 << 20) // math.isqrt(grade ** skew) + 1 for grade in range(2, number_of + 1)]
    spare, given = total - most - (number_of - 1), [1] * (number_of - 1)
    while spare > 0:
        free = [i for i in range(number_of - 1) if given[i] < most]
        whole, remaining = sum([portions[i] for i in free]), spare
        for i in free:
            addition = min(most - given[i], max(1, remaining * portions[i] // whole), spare)
            given[i] = given[i] + addition
            spare = spare - addition
    return np.array([most] + given)


def uneven_parts(own_key, amount, total, reach, lean):
    if amount == 2:
        one = jax.random.randint(own_key, (), max(1, total - reach), min(reach, total - 1) + 1)
        return jnp.stack([one, total - one])
    tallies = jnp.asarray(length_profile(amount, total, reach, lean), jnp.int32)
    twos = (amount - 1) // 2
    giver, taker = tallies[1:1 + 2 * twos:2], tallies[2:2 + 2 * twos:2]
    room = jnp.minimum(giver - 1, reach - taker)
    shifted = jax.random.randint(jax.random.fold_in(own_key, 1), (twos,), 0, 1 << 20) % (room + 1)
    tallies = tallies.at[1:1 + 2 * twos:2].set(giver - shifted).at[2:2 + 2 * twos:2].set(taker + shifted)
    return tallies[jax.random.permutation(jax.random.fold_in(own_key, 2), amount)]


def bell_draw(stream_key, extent, width, most, cuts=(), kind=jnp.bfloat16):
    drawn = jax.random.normal(stream_key, extent, jnp.float32) * width
    if len(cuts) > 0:
        drawn = steps_of(stream_key, extent, cuts, -0.22, 0.18) * drawn
    return jnp.clip(drawn, min=-most, max=most).astype(kind)


def setup_inputs(seed: int = 0) -> dict:
    splits = jax.random.split(jax.random.key(seed), 12)
    return {
        "patches": draw_patches(jax.random.fold_in(splits[11], 71), 0),
        "frames": jnp.searchsorted(jnp.cumsum(uneven_parts(splits[1], 2 * PATCHES // PAT_DEV, PATCHES, PAT_DEV, 1)), jnp.arange(PATCHES), side="right").astype(jnp.int32),
        "enc_qkv": bell_draw(splits[2], (3, ENC_WIDTH, ENC_WIDTH), ENC_WIDTH ** -0.5, 0.1875, ((2, 8),)),
        "enc_out": bell_draw(splits[3], (ENC_WIDTH, ENC_WIDTH), ENC_WIDTH ** -0.5, 0.1875, ((0, 8),)),
        "merge_gain": jnp.clip(1.0 + 0.1 * jax.random.normal(splits[4], (2, 4 * ENC_WIDTH), jnp.float32), 0.5, 1.5),
        "merge_w": bell_draw(splits[5], (2, 4 * ENC_WIDTH, WIDTH), (4 * ENC_WIDTH) ** -0.5, 0.09375, ((1, 32), (2, 8))),
        "embedded": draw_embedded(jax.random.fold_in(splits[11], 71), 0),
        "source": draw_source(jax.random.fold_in(splits[11], 71), 0),
        "dec_q": bell_draw(splits[8], (WIDTH, Q_HEADS * HEAD_DIM), WIDTH ** -0.5, 0.078125, ((0, 32), (1, 8))),
        "dec_kv": bell_draw(splits[9], (WIDTH, 2 * KV_HEADS * HEAD_DIM), WIDTH ** -0.5, 0.078125, ((0, 32), (1, 8))),
        "cotangent": bell_draw(splits[10], (TOKENS, 2, WIDTH), 1.0, 6.0, ((0, 32), (2, 8))),
    }


def rms_rows(rows, gain):
    wide = rows.astype(jnp.float32)
    mean_sq = lax.optimization_barrier(jnp.mean(wide * wide, axis=-1, keepdims=True))
    return wide * lax.rsqrt(mean_sq + 1e-06) * gain

def reference(patches, frames, enc_qkv, enc_out, merge_gain, merge_w, embedded, source, dec_q, dec_kv, cotangent):
    enc_dim = ENC_WIDTH // ENC_HEADS
    enc_q = jnp.dot(patches, enc_qkv[0], preferred_element_type=jnp.float32).astype(jnp.bfloat16)
    enc_k = jnp.dot(patches, enc_qkv[1], preferred_element_type=jnp.float32).astype(jnp.bfloat16)
    enc_v = jnp.dot(patches, enc_qkv[2], preferred_element_type=jnp.float32).astype(jnp.bfloat16)
    same = frames[:, None] == frames[None, :]

    def enc_head(index):
        start = (index * enc_dim).astype(jnp.int32)
        query = lax.dynamic_slice_in_dim(enc_q, start, enc_dim, 1)
        keys = lax.dynamic_slice_in_dim(enc_k, start, enc_dim, 1)
        values = lax.dynamic_slice_in_dim(enc_v, start, enc_dim, 1)
        scores = jnp.dot(query, keys.T, preferred_element_type=jnp.float32) / jnp.sqrt(jnp.float32(enc_dim))
        scores = jnp.where(same, scores, jnp.float32(-1e+30))
        top = lax.optimization_barrier(jnp.max(scores, axis=1, keepdims=True))
        weights = jnp.where(same, jnp.exp(scores - top), jnp.float32(0.0))
        total = lax.optimization_barrier(jnp.sum(weights, axis=1, keepdims=True))
        mixed = jnp.dot(weights.astype(jnp.bfloat16), values, preferred_element_type=jnp.float32)
        return (mixed / total).astype(jnp.bfloat16)
    heads_out = lax.map(enc_head, jnp.arange(ENC_HEADS, dtype=jnp.int32))
    enc_attn = jnp.transpose(heads_out, (1, 0, 2)).reshape(PATCHES, ENC_WIDTH)
    enc_hidden = (patches.astype(jnp.float32) + jnp.dot(enc_attn, enc_out, preferred_element_type=jnp.float32)).astype(jnp.bfloat16)
    levels = [patches.reshape(MERGED, 4 * ENC_WIDTH), enc_hidden.reshape(MERGED, 4 * ENC_WIDTH)]
    merged_list = []
    for level in range(2):
        normed = rms_rows(levels[level], merge_gain[level]).astype(jnp.bfloat16)
        merged_list.append(jnp.dot(normed, merge_w[level], preferred_element_type=jnp.float32).astype(jnp.bfloat16))
    merged = jnp.stack(merged_list)
    index = jnp.clip(source, 0, MERGED - 1).astype(jnp.int32)
    inject = jnp.where(source[:, None] >= 0, merged[0][index].astype(jnp.float32), jnp.float32(0.0))
    states = (embedded.astype(jnp.float32) + inject).astype(jnp.bfloat16)
    queries = jnp.dot(states, dec_q, preferred_element_type=jnp.float32).astype(jnp.bfloat16)
    keys_values = jnp.dot(states, dec_kv, preferred_element_type=jnp.float32).astype(jnp.bfloat16)
    positions = jnp.arange(TOKENS, dtype=jnp.int32)
    causal = positions[:, None] >= positions[None, :]
    group = Q_HEADS // KV_HEADS

    def dec_head(head):
        kv_head = head // group
        query = lax.dynamic_slice_in_dim(queries, (head * HEAD_DIM).astype(jnp.int32), HEAD_DIM, 1)
        keys = lax.dynamic_slice_in_dim(keys_values, (kv_head * 2 * HEAD_DIM).astype(jnp.int32), HEAD_DIM, 1)
        values = lax.dynamic_slice_in_dim(keys_values, (kv_head * 2 * HEAD_DIM + HEAD_DIM).astype(jnp.int32), HEAD_DIM, 1)
        scores = jnp.dot(query, keys.T, preferred_element_type=jnp.float32) / jnp.sqrt(jnp.float32(HEAD_DIM))
        scores = jnp.where(causal, scores, jnp.float32(-1e+30))
        top = lax.optimization_barrier(jnp.max(scores, axis=1, keepdims=True))
        weights = jnp.where(causal, jnp.exp(scores - top), jnp.float32(0.0))
        total = lax.optimization_barrier(jnp.sum(weights, axis=1, keepdims=True))
        mixed = jnp.dot(weights.astype(jnp.bfloat16), values, preferred_element_type=jnp.float32)
        return (mixed / total).astype(jnp.bfloat16)
    dec_out = lax.map(dec_head, jnp.arange(Q_HEADS, dtype=jnp.int32))
    context = jnp.transpose(dec_out, (1, 0, 2)).reshape(TOKENS, Q_HEADS * HEAD_DIM)
    picker = (source[None, :] == jnp.arange(MERGED, dtype=jnp.int32)[:, None]).astype(jnp.bfloat16)
    level_grads = jnp.stack([jnp.dot(picker, cotangent[:, level, :], preferred_element_type=jnp.float32) for level in range(2)])
    return (merged, context, level_grads)
```

```python
import jax
import jax.numpy as jnp
from jax import lax
from jax.experimental import pallas as pl
from jax.experimental.pallas import tpu as pltpu
from jax.sharding import Mesh, PartitionSpec as P

ENC_HEADS = 16
HEAD_DIM = 128
RETURN_MOST = 4
PL = ("c", "z", "xl")
HD = ("xh", "y")
F32 = jnp.float32
BF16 = jnp.bfloat16


def axis_len(axes):
    return lax.axis_size(axes)


def exchange(tiles, axes):
    return lax.all_to_all(tiles, axes, 0, 0, tiled=True)


def from_everyone(value, axes):
    return exchange(jnp.broadcast_to(value[None], (axis_len(axes), *value.shape)), axes)


def in_order(tiles):
    return jnp.moveaxis(tiles, 0, 1).reshape(tiles.shape[1], -1)


def swapped(value, axis):
    return lax.ppermute(value, axis, [(0, 1), (1, 0)])


def shifted(value, axis, by):
    n = axis_len(axis)
    return lax.ppermute(value, axis, [(i, (i + by) % n) for i in range(n)])


def dot(a, b):
    return jnp.dot(a, b, preferred_element_type=F32)


def attend(q, keys, values, mask, state):
    s = lax.dot_general(keys, q, (((1,), (1,)), ((), ())), preferred_element_type=F32)
    if mask is not None:
        s = jnp.where(mask, s, F32(-1e30))
    factor = F32(1.4426950408889634 / HEAD_DIM**0.5)
    top = jnp.max(s, axis=0, keepdims=True)
    if state is not None:
        top = jnp.maximum(state[0], top)
    p = jnp.exp2((s - top) * factor)
    total = jnp.sum(p, axis=0, keepdims=True)
    mixed = lax.dot_general(
        values, p.astype(BF16), (((0,), (0,)), ((), ())), preferred_element_type=F32
    )
    if state is not None:
        keep = jnp.exp2((state[0] - top) * factor)
        total = total + state[1] * keep
        mixed = mixed + state[2] * keep
    return top, total, mixed


def attention_kernel(info, q_ref, own_ref, near_ref, far_ref, out_ref, m_ref, l_ref, acc_ref):
    rows = q_ref.shape[0]
    group = q_ref.shape[1] // HEAD_DIM
    blocks = near_ref.shape[0]
    z, c, xl = info[0], info[1], info[2]

    def heads(block, mask, first):
        keys, values = block[:, :HEAD_DIM], block[:, HEAD_DIM:]
        for h in range(group):
            q = q_ref[:, h * HEAD_DIM : (h + 1) * HEAD_DIM]
            state = None if first else (m_ref[h], l_ref[h], acc_ref[h])
            m_ref[h], l_ref[h], acc_ref[h] = attend(q, keys, values, mask, state)

    key = lax.broadcasted_iota(jnp.int32, (2 * rows, rows), 0)
    query = lax.broadcasted_iota(jnp.int32, (2 * rows, rows), 1)
    limit = jnp.where(xl == 1, 2 * rows, 0)
    mask = (key <= query) | ((key >= rows) & (key < limit))
    heads(own_ref[...], mask, True)

    def near_step(i, _):
        @pl.when(info[3 + i] == 1)
        def _():
            heads(near_ref[i], None, False)

        return 0

    lax.fori_loop(0, blocks, near_step, 0)

    @pl.when(c == 1)
    def _():
        def far_step(i, _):
            heads(far_ref[i], None, False)
            return 0

        lax.fori_loop(0, far_ref.shape[0], far_step, 0)

    for h in range(group):
        out = acc_ref[h] / l_ref[h]
        out_ref[:, h * HEAD_DIM : (h + 1) * HEAD_DIM] = out.T.astype(BF16)


def attention(info, q, own, near, far):
    rows, cols = q.shape
    group = cols // HEAD_DIM
    vm = pl.BlockSpec(memory_space=pltpu.VMEM)
    return pl.pallas_call(
        attention_kernel,
        out_shape=jax.ShapeDtypeStruct((rows, cols), BF16),
        in_specs=[pl.BlockSpec(memory_space=pltpu.SMEM), vm, vm, vm, vm],
        out_specs=vm,
        scratch_shapes=[
            pltpu.VMEM((group, 1, rows), F32),
            pltpu.VMEM((group, 1, rows), F32),
            pltpu.VMEM((group, HEAD_DIM, rows), F32),
        ],
        compiler_params=pltpu.CompilerParams(vmem_limit_bytes=48 * 1024 * 1024),
        name="causal_attention",
    )(info, q, own, near, far)


def merged_level(tiles, gain, weights):
    heads, rows, cols = tiles.shape
    r = rows // 4
    wide = tiles.astype(F32).reshape(heads, 4, r, cols)
    count = heads * 4 * cols
    mean_sq = jnp.sum(wide * wide, axis=(0, 1, 3), keepdims=True) / count
    g = jnp.transpose(gain.reshape(4, heads, cols), (1, 0, 2))[:, :, None, :]
    normed = (wide * lax.rsqrt(mean_sq + 1e-06) * g).astype(BF16)
    zn = axis_len("z")
    lo = zn // 2
    split = normed.reshape(lo, 2, 2, 2, r, cols)
    send = jnp.transpose(split, (3, 0, 2, 1, 4, 5)).reshape(zn, 4, r, cols)
    got = exchange(send, "z")
    part = sum(
        dot(got[:, k].reshape(zn * r, cols), weights[k]) for k in range(4)
    )
    back = exchange(part.astype(BF16).reshape(zn, r, -1), "z")
    return back.astype(F32).sum(axis=0).astype(BF16)


def shards(
    patches, frames, enc_qkv, enc_out, merge_gain, merge_w, embedded, source, dec_q, dec_kv, cotangent
):
    place = lax.axis_index(PL)
    z, c, xl = lax.axis_index("z"), lax.axis_index("c"), lax.axis_index("xl")
    pat_rows = patches.shape[0]
    tok_rows = embedded.shape[0]
    merged_rows = pat_rows // 4
    places = axis_len(PL)

    dec_w = lax.all_gather(jnp.concatenate([dec_q, dec_kv], axis=1), PL, axis=0, tiled=True)

    new = jnp.arange(pat_rows, dtype=jnp.int32)
    old = (new % merged_rows) * 4 + new // merged_rows
    reorder = (old[:, None] == jnp.arange(pat_rows, dtype=jnp.int32)[None, :]).astype(BF16)
    mine = dot(reorder, patches).astype(BF16)
    tiles = from_everyone(mine, HD)

    visual = source >= 0
    holder = jnp.where(visual, source // merged_rows, -1)
    row_ids = jnp.arange(tok_rows, dtype=jnp.int32)
    before = row_ids[None, :] < row_ids[:, None]
    earlier = (holder[:, None] == holder[None, :]) & before
    order_rank = jnp.sum(earlier.astype(jnp.int32), axis=1)
    bucket_slot = jnp.where(visual, holder * RETURN_MOST + order_rank, -1)
    slots = places * RETURN_MOST
    placer = jnp.arange(slots, dtype=jnp.int32)[:, None] == bucket_slot[None, :]
    bucket_ids = jnp.sum(jnp.where(placer, source[None, :] + 1, 0), axis=1) - 1
    arrived_ids = exchange(bucket_ids, PL)
    local_index = arrived_ids - place * merged_rows
    setter = (
        jnp.arange(merged_rows, dtype=jnp.int32)[:, None] == local_index[None, :]
    ).astype(BF16)

    w0 = from_everyone(merge_w[0], ("c", "xl"))
    w1 = from_everyone(merge_w[1], ("c", "xl"))
    merged0 = merged_level(tiles, merge_gain[0], w0)

    to_send = dot(setter.T, merged0).astype(BF16)
    taken = exchange(to_send, PL)
    vis_rank = jnp.sum((visual[None, :] & before).astype(jnp.int32), axis=1)
    chosen = visual[None, :] & (
        jnp.arange(merged_rows, dtype=jnp.int32)[:, None] == vis_rank[None, :]
    )
    slot_of = jnp.sum(jnp.where(chosen, bucket_slot[None, :] + 1, 0), axis=1) - 1
    fetch = (slot_of[:, None] == jnp.arange(slots, dtype=jnp.int32)[None, :]).astype(BF16)
    inject = dot(fetch, taken)
    chosen_bf = chosen.astype(BF16)
    vis_states = (dot(chosen_bf, embedded) + inject).astype(BF16)

    emb_full = in_order(from_everyone(embedded, HD))
    vis_full = in_order(from_everyone(vis_states, HD))
    text_proj = dot(emb_full, dec_w).astype(BF16)
    vis_proj = dot(vis_full, dec_w).astype(BF16)
    placed = dot(chosen_bf.T, vis_proj)
    proj = jnp.where(visual[:, None], placed, text_proj.astype(F32)).astype(BF16)
    query_cols = dec_q.shape[1]
    queries, kv = proj[:, :query_cols], proj[:, query_cols:]

    pair = jnp.concatenate([kv, swapped(kv, "xl")], axis=0)
    zn = axis_len("z")
    up, down = [pair], [pair]
    near, away = [], []
    for step in range(1, zn // 2 + 1):
        up.append(shifted(up[-1], "z", 1))
        near.append(up[-1])
        away.append(-step)
        if step < zn // 2:
            down.append(shifted(down[-1], "z", -1))
            near.append(down[-1])
            away.append(step)
    far = [swapped(b, "c") for b in [pair] + near]
    seen = [((z + a) % zn < z).astype(jnp.int32) for a in away]
    info = jnp.stack([z, c, xl] + seen).astype(jnp.int32)
    context = attention(info, queries, pair, jnp.stack(near), jnp.stack(far))

    full_patches = in_order(tiles)
    local_cols = enc_qkv.shape[2]
    enc_dim = full_patches.shape[1] // ENC_HEADS
    local_heads = local_cols // enc_dim
    enc_q = dot(full_patches, enc_qkv[0]).astype(BF16)
    enc_k = dot(full_patches, enc_qkv[1]).astype(BF16)
    enc_v = dot(full_patches, enc_qkv[2]).astype(BF16)
    paired = jnp.concatenate([enc_k, enc_v], axis=1)
    upward = [(i, i + 1) for i in range(places - 1)]
    low = lax.ppermute(paired, PL, upward)
    high = lax.ppermute(paired, PL, [(b, a) for a, b in upward])
    widened = jnp.concatenate([low, paired, high], axis=0)
    padded = jnp.pad(frames, (pat_rows, pat_rows), constant_values=-1)
    key_frames = lax.dynamic_slice_in_dim(padded, place * pat_rows, 3 * pat_rows)
    key_frames = jnp.swapaxes(key_frames.reshape(3, merged_rows, 4), 1, 2).reshape(-1)
    own_frames = key_frames[pat_rows : 2 * pat_rows]
    same = own_frames[:, None] == key_frames[None, :]
    query3 = enc_q.reshape(pat_rows, local_heads, enc_dim)
    keys3 = widened[:, :local_cols].reshape(3 * pat_rows, local_heads, enc_dim)
    values3 = widened[:, local_cols:].reshape(3 * pat_rows, local_heads, enc_dim)
    scores = jnp.einsum("qhd,khd->hqk", query3, keys3, preferred_element_type=F32) / jnp.sqrt(
        F32(enc_dim)
    )
    scores = jnp.where(same[None], scores, F32(-1e30))
    top = jnp.max(scores, axis=2, keepdims=True)
    weights = jnp.where(same[None], jnp.exp(scores - top), F32(0.0))
    total = jnp.sum(weights, axis=2)
    mixed = jnp.einsum("hqk,khd->qhd", weights.astype(BF16), values3, preferred_element_type=F32)
    enc_attn = (
        (mixed / jnp.transpose(total)[:, :, None]).astype(BF16).reshape(pat_rows, local_cols)
    )
    partial_out = dot(enc_attn, enc_out).astype(BF16)
    heads = axis_len(HD)
    outs = jnp.moveaxis(partial_out.reshape(pat_rows, heads, local_cols), 1, 0)
    summed = exchange(outs, HD).astype(F32).sum(axis=0)
    enc_hidden = (mine.astype(F32) + summed).astype(BF16)
    merged1 = merged_level(from_everyone(enc_hidden, HD), merge_gain[1], w1)

    cot_flat = cotangent.reshape(tok_rows, 2 * cotangent.shape[2])
    bucket_rows = dot(placer.astype(BF16), cot_flat).astype(BF16)
    arrived_rows = exchange(bucket_rows, PL)
    returned = dot(setter, arrived_rows)
    level_grads = jnp.transpose(returned.reshape(merged_rows, 2, cotangent.shape[2]), (1, 0, 2))
    return jnp.stack([merged0, merged1]), context, level_grads


def solution(mesh):
    fine = Mesh(mesh.devices.reshape(2, 8, 2, 2, 4), ("c", "z", "xl", "xh", "y"))
    in_specs = (
        P(PL, HD),
        P(),
        P(None, None, HD),
        P(HD, None),
        P(),
        P(None, PL, HD),
        P(PL, HD),
        P(PL),
        P(PL, HD),
        P(PL, HD),
        P(PL, None, HD),
    )
    out_specs = (P(None, PL, HD), P(PL, HD), P(None, PL, HD))
    return jax.shard_map(shards, mesh=fine, in_specs=in_specs, out_specs=out_specs, check_vma=False)
```

```python
import jax
import jax.numpy as jnp
from jax import lax
from jax.experimental import pallas as pl
from jax.experimental.pallas import tpu as pltpu
from jax.sharding import Mesh, PartitionSpec as P

ENC_HEADS = 16
HEAD_DIM = 128
RETURN_MOST = 4
PL = ("c", "z", "xl")
HD = ("xh", "y")
F32 = jnp.float32
BF16 = jnp.bfloat16


def axis_len(axes):
    return lax.axis_size(axes)


def exchange(tiles, axes):
    return lax.all_to_all(tiles, axes, 0, 0, tiled=True)


def from_everyone(value, axes):
    return exchange(jnp.broadcast_to(value[None], (axis_len(axes), *value.shape)), axes)


def in_order(tiles):
    return jnp.moveaxis(tiles, 0, 1).reshape(tiles.shape[1], -1)


def swapped(value, axis):
    return lax.ppermute(value, axis, [(0, 1), (1, 0)])


def shifted(value, axis, by):
    n = axis_len(axis)
    return lax.ppermute(value, axis, [(i, (i + by) % n) for i in range(n)])


def dot(a, b):
    return jnp.dot(a, b, preferred_element_type=F32)


FACTOR = 1.4426950408889634 / HEAD_DIM**0.5
CHUNK = 64


def take_block(q_ref, block, mask, m_ref, l_ref, acc_ref, s_ref, p_ref):
    keys, values = block[:, :HEAD_DIM], block[:, HEAD_DIM:]
    count, rows = keys.shape[0], q_ref.shape[0]
    group = q_ref.shape[1] // HEAD_DIM
    first = mask is not None
    turned = values.T
    for h in range(group):
        q = q_ref[:, h * HEAD_DIM : (h + 1) * HEAD_DIM]
        s_ref[h] = lax.dot_general(keys, q, (((1,), (1,)), ((), ())), preferred_element_type=F32)
    for h in range(group):
        top = None
        for i in range(0, count, CHUNK):
            s = s_ref[h, i : i + CHUNK]
            if first:
                s = jnp.where(mask(i), s, F32(-1e30))
                s_ref[h, i : i + CHUNK] = s
            t = jnp.max(s.reshape(CHUNK // 8, 8, rows), axis=0)
            top = t if top is None else jnp.maximum(top, t)
        top = jnp.max(top, axis=0, keepdims=True)
        if not first:
            top = jnp.maximum(m_ref[h], top)
        total = None
        for i in range(0, count, CHUNK):
            p = jnp.exp2((s_ref[h, i : i + CHUNK] - top) * F32(FACTOR))
            t = jnp.sum(p.reshape(CHUNK // 8, 8, rows), axis=0)
            total = t if total is None else total + t
            p_ref[h, i : i + CHUNK] = p.astype(BF16)
        total = jnp.sum(total, axis=0, keepdims=True)
        mixed = jnp.dot(turned, p_ref[h], preferred_element_type=F32)
        if not first:
            keep = jnp.exp2((m_ref[h] - top) * F32(FACTOR))
            total = total + l_ref[h] * keep
            mixed = mixed + acc_ref[h] * keep
        m_ref[h], l_ref[h], acc_ref[h] = top, total, mixed


def attention_kernel(info, q_ref, own_ref, rest_ref, out_ref, *scratch):
    rows = q_ref.shape[0]
    group = q_ref.shape[1] // HEAD_DIM
    limit = jnp.where(info[0] == 1, 2 * rows, 0)

    def mask(start):
        key = lax.broadcasted_iota(jnp.int32, (CHUNK, rows), 0) + start
        query = lax.broadcasted_iota(jnp.int32, (CHUNK, rows), 1)
        return (key <= query) | ((key >= rows) & (key < limit))

    take_block(q_ref, own_ref[...], mask, *scratch)

    def step(i, _):
        @pl.when(info[1 + i] == 1)
        def _():
            take_block(q_ref, rest_ref[i], None, *scratch)

        return 0

    lax.fori_loop(0, rest_ref.shape[0], step, 0)

    acc_ref, l_ref = scratch[2], scratch[1]
    for h in range(group):
        out = acc_ref[h] / l_ref[h]
        out_ref[:, h * HEAD_DIM : (h + 1) * HEAD_DIM] = out.T.astype(BF16)


def attention(info, q, own, rest):
    rows, cols = q.shape
    group = cols // HEAD_DIM
    count = own.shape[0]
    vm = pl.BlockSpec(memory_space=pltpu.VMEM)
    return pl.pallas_call(
        attention_kernel,
        out_shape=jax.ShapeDtypeStruct((rows, cols), BF16),
        in_specs=[pl.BlockSpec(memory_space=pltpu.SMEM), vm, vm, vm],
        out_specs=vm,
        scratch_shapes=[
            pltpu.VMEM((group, 1, rows), F32),
            pltpu.VMEM((group, 1, rows), F32),
            pltpu.VMEM((group, HEAD_DIM, rows), F32),
            pltpu.VMEM((group, count, rows), F32),
            pltpu.VMEM((group, count, rows), BF16),
        ],
        compiler_params=pltpu.CompilerParams(vmem_limit_bytes=48 * 1024 * 1024),
        name="causal_attention",
    )(info, q, own, rest)


def gathered_apart(value, axes):
    n, me = axis_len(axes), lax.axis_index(axes)
    done = jnp.zeros((n, *value.shape), value.dtype)
    for step in range(n):
        piece = value
        if step:
            piece = lax.ppermute(value, axes, [(i, i ^ step) for i in range(n)])
        done = lax.dynamic_update_index_in_dim(done, piece, me ^ step, 0)
    return done


def normed_tiles(tiles, gain):
    heads, rows, cols = tiles.shape
    r = rows // 4
    wide = tiles.astype(F32).reshape(heads, 4, r, cols)
    count = heads * 4 * cols
    mean_sq = jnp.sum(wide * wide, axis=(0, 1, 3), keepdims=True) / count
    g = jnp.transpose(gain.reshape(4, heads, cols), (1, 0, 2))[:, :, None, :]
    normed = (wide * lax.rsqrt(mean_sq + 1e-06) * g).astype(BF16)
    zn = axis_len("z")
    split = normed.reshape(zn // 2, 2, 2, 2, r, cols)
    return jnp.transpose(split, (3, 0, 2, 1, 4, 5)).reshape(zn, 4, r, cols)


def projected(got, weights):
    zn, k, r, cols = got.shape
    part = sum(dot(got[:, i].reshape(zn * r, cols), weights[i]) for i in range(k))
    back = exchange(part.astype(BF16).reshape(zn, r, -1), "z")
    return back.astype(F32).sum(axis=0).astype(BF16)


def shards(
    patches, frames, enc_qkv, enc_out, merge_gain, merge_w, embedded, source, dec_q, dec_kv, cotangent
):
    place = lax.axis_index(PL)
    z, c, xl = lax.axis_index("z"), lax.axis_index("c"), lax.axis_index("xl")
    pat_rows, pat_cols = patches.shape
    tok_rows = embedded.shape[0]
    merged_rows = pat_rows // 4
    places = axis_len(PL)
    zn = axis_len("z")

    dec_w = lax.all_gather(jnp.concatenate([dec_q, dec_kv], axis=1), PL, axis=0, tiled=True)

    new = jnp.arange(pat_rows, dtype=jnp.int32)
    old = (new % merged_rows) * 4 + new // merged_rows
    reorder = (old[:, None] == jnp.arange(pat_rows, dtype=jnp.int32)[None, :]).astype(BF16)
    mine = dot(reorder, patches).astype(BF16)
    tiles = from_everyone(mine, HD)
    w_all = gathered_apart(merge_w, ("c", "xl"))
    sources = gathered_apart(source, ("c", "xl")) + 1
    embedded_late, enc_out_late, _ = lax.optimization_barrier((embedded, enc_out, tiles))

    coded = jnp.stack([sources // 64, sources % 64], axis=1).astype(BF16)
    coded = coded.reshape(4, merged_rows, -1)
    send = normed_tiles(tiles, merge_gain[0])
    send = jnp.concatenate([send, jnp.broadcast_to(coded[None], (zn, *coded.shape))], axis=3)
    got = exchange(send, "z")
    merged0 = projected(got[..., :pat_cols], w_all[:, 0])
    codes = got[..., pat_cols:].astype(jnp.int32).reshape(zn, 2, 2, 2, tok_rows)
    codes = codes[:, :, :, 0] * 64 + codes[:, :, :, 1] - 1
    all_source = jnp.transpose(codes, (1, 0, 2, 3)).reshape(places, tok_rows)

    row_ids = jnp.arange(tok_rows, dtype=jnp.int32)
    before = row_ids[:, None] < row_ids[None, :]
    wanted = (all_source >= 0) & (all_source // merged_rows == place)
    rank = dot(wanted.astype(BF16), before.astype(BF16)).astype(jnp.int32)
    rank = jnp.where(wanted, rank, -1)
    slot_ids = jnp.arange(RETURN_MOST, dtype=jnp.int32)
    local = jnp.sum(
        jnp.where(
            rank[:, None, :] == slot_ids[None, :, None], all_source[:, None, :] % merged_rows + 1, 0
        ),
        axis=2,
    ).reshape(-1) - 1
    merged_ids = jnp.arange(merged_rows, dtype=jnp.int32)
    setter = (merged_ids[:, None] == local[None, :]).astype(BF16)

    visual = source >= 0
    holder = jnp.where(visual, source // merged_rows, -1)
    earlier = (holder[:, None] == holder[None, :]) & before.T
    order_rank = jnp.sum(earlier.astype(jnp.int32), axis=1)
    bucket_slot = jnp.where(visual, holder * RETURN_MOST + order_rank, -1)
    slots = places * RETURN_MOST
    placer = jnp.arange(slots, dtype=jnp.int32)[:, None] == bucket_slot[None, :]
    vis_rank = jnp.sum((visual[None, :] & before.T).astype(jnp.int32), axis=1)
    chosen = visual[None, :] & (merged_ids[:, None] == vis_rank[None, :])
    slot_of = jnp.sum(jnp.where(chosen, bucket_slot[None, :] + 1, 0), axis=1) - 1
    fetch = (slot_of[:, None] == jnp.arange(slots, dtype=jnp.int32)[None, :]).astype(BF16)
    chosen_bf = chosen.astype(BF16)

    taken = exchange(dot(setter.T, merged0).astype(BF16), PL)
    vis_states = (dot(chosen_bf, embedded) + dot(fetch, taken)).astype(BF16)
    vis_tiles = from_everyone(vis_states, HD)

    emb_tiles = gathered_apart(embedded_late, HD)
    placed = jnp.einsum("vr,hvc->hrc", chosen_bf, vis_tiles, preferred_element_type=F32)
    states = jnp.where(visual[None, :, None], placed.astype(BF16), emb_tiles)
    states = in_order(states)
    query_cols = dec_q.shape[1]
    kv = dot(states, dec_w[:, query_cols:]).astype(BF16)
    queries = dot(states, dec_w[:, :query_cols]).astype(BF16)

    pair = jnp.concatenate([kv, swapped(kv, "xl")], axis=0)
    up, down = [pair], [pair]
    near, away = [], []
    for step in range(1, zn // 2 + 1):
        up.append(shifted(up[-1], "z", 1))
        near.append(up[-1])
        away.append(-step)
        if step < zn // 2:
            down.append(shifted(down[-1], "z", -1))
            near.append(down[-1])
            away.append(step)
    far = [swapped(b, "c") for b in [pair] + near]
    seen = [((z + a) % zn < z).astype(jnp.int32) for a in away]
    info = jnp.stack([xl] + seen + [c] * len(far)).astype(jnp.int32)
    context = attention(info, queries, pair, jnp.stack(near + far))

    full_patches = in_order(tiles)
    local_cols = enc_qkv.shape[2]
    enc_dim = full_patches.shape[1] // ENC_HEADS
    local_heads = local_cols // enc_dim
    enc_q = dot(full_patches, enc_qkv[0]).astype(BF16)
    enc_k = dot(full_patches, enc_qkv[1]).astype(BF16)
    enc_v = dot(full_patches, enc_qkv[2]).astype(BF16)
    paired = jnp.concatenate([enc_k, enc_v], axis=1)
    upward = [(i, i + 1) for i in range(places - 1)]
    low = lax.ppermute(paired, PL, upward)
    high = lax.ppermute(paired, PL, [(b, a) for a, b in upward])
    widened = jnp.concatenate([low, paired, high], axis=0)
    padded = jnp.pad(frames, (pat_rows, pat_rows), constant_values=-1)
    key_frames = lax.dynamic_slice_in_dim(padded, place * pat_rows, 3 * pat_rows)
    key_frames = jnp.swapaxes(key_frames.reshape(3, merged_rows, 4), 1, 2).reshape(-1)
    own_frames = key_frames[pat_rows : 2 * pat_rows]
    same = own_frames[:, None] == key_frames[None, :]
    query3 = enc_q.reshape(pat_rows, local_heads, enc_dim)
    keys3 = widened[:, :local_cols].reshape(3 * pat_rows, local_heads, enc_dim)
    values3 = widened[:, local_cols:].reshape(3 * pat_rows, local_heads, enc_dim)
    scores = jnp.einsum("qhd,khd->hqk", query3, keys3, preferred_element_type=F32) / jnp.sqrt(
        F32(enc_dim)
    )
    scores = jnp.where(same[None], scores, F32(-1e30))
    top = jnp.max(scores, axis=2, keepdims=True)
    weights = jnp.where(same[None], jnp.exp(scores - top), F32(0.0))
    total = jnp.sum(weights, axis=2)
    mixed = jnp.einsum("hqk,khd->qhd", weights.astype(BF16), values3, preferred_element_type=F32)
    enc_attn = (
        (mixed / jnp.transpose(total)[:, :, None]).astype(BF16).reshape(pat_rows, local_cols)
    )
    enc_attn, _ = lax.optimization_barrier((enc_attn, kv))
    out_w = gathered_apart(enc_out_late, HD).reshape(-1, enc_out.shape[1])
    full_attn = in_order(from_everyone(enc_attn, HD))
    full_hidden = (full_patches.astype(F32) + dot(full_attn, out_w)).astype(BF16)
    hidden_tiles = jnp.moveaxis(full_hidden.reshape(pat_rows, -1, pat_cols), 1, 0)
    got1 = exchange(normed_tiles(hidden_tiles, merge_gain[1]), "z")
    merged1 = projected(got1, w_all[:, 1])

    cot_flat = cotangent.reshape(tok_rows, 2 * cotangent.shape[2])
    bucket_rows = dot(placer.astype(BF16), cot_flat).astype(BF16)
    bucket_rows, _ = lax.optimization_barrier((bucket_rows, merged1))
    arrived_rows = exchange(bucket_rows, PL)
    returned = dot(setter, arrived_rows)
    level_grads = jnp.transpose(returned.reshape(merged_rows, 2, cotangent.shape[2]), (1, 0, 2))
    return jnp.stack([merged0, merged1]), context, level_grads


def solution(mesh):
    fine = Mesh(mesh.devices.reshape(2, 8, 2, 2, 4), ("c", "z", "xl", "xh", "y"))
    in_specs = (
        P(PL, HD),
        P(),
        P(None, None, HD),
        P(HD, None),
        P(),
        P(None, PL, HD),
        P(PL, HD),
        P(PL),
        P(PL, HD),
        P(PL, HD),
        P(PL, None, HD),
    )
    out_specs = (P(None, PL, HD), P(PL, HD), P(None, PL, HD))
    return jax.shard_map(shards, mesh=fine, in_specs=in_specs, out_specs=out_specs, check_vma=False)
```

```python
import functools

import jax
import jax.numpy as jnp
from jax import lax
from jax.experimental import pallas as pl
from jax.experimental.pallas import tpu as pltpu
from jax.sharding import Mesh, PartitionSpec as P

ENC_HEADS = 16
HEAD_DIM = 128
RETURN_MOST = 4
PL = ("c", "z", "xl")
HD = ("xh", "y")
F32 = jnp.float32
BF16 = jnp.bfloat16


def axis_len(axes):
    return lax.axis_size(axes)


def exchange(tiles, axes):
    return lax.all_to_all(tiles, axes, 0, 0, tiled=True)


def from_everyone(value, axes):
    return exchange(jnp.broadcast_to(value[None], (axis_len(axes), *value.shape)), axes)


def in_order(tiles):
    return jnp.moveaxis(tiles, 0, 1).reshape(tiles.shape[1], -1)


def swapped(value, axis):
    return lax.ppermute(value, axis, [(0, 1), (1, 0)])


def shifted(value, axis, by):
    n = axis_len(axis)
    return lax.ppermute(value, axis, [(i, (i + by) % n) for i in range(n)])


def dot(a, b):
    return jnp.dot(a, b, preferred_element_type=F32)


FACTOR = 1.4426950408889634 / HEAD_DIM**0.5
CHUNK = 64


def take_block(q_ref, block, mask, m_ref, l_ref, acc_ref, s_ref, p_ref):
    keys, values = block[:, :HEAD_DIM], block[:, HEAD_DIM:]
    count, rows = keys.shape[0], q_ref.shape[0]
    group = q_ref.shape[1] // HEAD_DIM
    first = mask is not None
    turned = values.T
    for h in range(group):
        q = q_ref[:, h * HEAD_DIM : (h + 1) * HEAD_DIM]
        s_ref[h] = lax.dot_general(keys, q, (((1,), (1,)), ((), ())), preferred_element_type=F32)
    for h in range(group):
        top = None
        for i in range(0, count, CHUNK):
            s = s_ref[h, i : i + CHUNK]
            if first:
                s = jnp.where(mask(i), s, F32(-1e30))
                s_ref[h, i : i + CHUNK] = s
            t = jnp.max(s.reshape(CHUNK // 8, 8, rows), axis=0)
            top = t if top is None else jnp.maximum(top, t)
        top = jnp.max(top, axis=0, keepdims=True)
        if not first:
            top = jnp.maximum(m_ref[h], top)
        total = None
        for i in range(0, count, CHUNK):
            p = jnp.exp2((s_ref[h, i : i + CHUNK] - top) * F32(FACTOR))
            t = jnp.sum(p.reshape(CHUNK // 8, 8, rows), axis=0)
            total = t if total is None else total + t
            p_ref[h, i : i + CHUNK] = p.astype(BF16)
        total = jnp.sum(total, axis=0, keepdims=True)
        mixed = jnp.dot(turned, p_ref[h], preferred_element_type=F32)
        if not first:
            keep = jnp.exp2((m_ref[h] - top) * F32(FACTOR))
            total = total + l_ref[h] * keep
            mixed = mixed + acc_ref[h] * keep
        m_ref[h], l_ref[h], acc_ref[h] = top, total, mixed


def attention_kernel(info, q_ref, own_ref, *refs):
    rest, out_ref, buffer, scratch = refs[:-7], refs[-7], refs[-6], refs[-5:]
    rows = q_ref.shape[0]
    group = q_ref.shape[1] // HEAD_DIM
    limit = jnp.where(info[0] == 1, 2 * rows, 0)

    def mask(start):
        key = lax.broadcasted_iota(jnp.int32, (CHUNK, rows), 0) + start
        query = lax.broadcasted_iota(jnp.int32, (CHUNK, rows), 1)
        return (key <= query) | ((key >= rows) & (key < limit))

    for i, ref in enumerate(rest):
        buffer[i] = ref[...]
    take_block(q_ref, own_ref[...], mask, *scratch)

    def step(i, _):
        @pl.when(info[1 + i] == 1)
        def _():
            take_block(q_ref, buffer[i], None, *scratch)

        return 0

    lax.fori_loop(0, len(rest), step, 0)

    acc_ref, l_ref = scratch[2], scratch[1]
    for h in range(group):
        out = acc_ref[h] / l_ref[h]
        out_ref[:, h * HEAD_DIM : (h + 1) * HEAD_DIM] = out.T.astype(BF16)


VMEM = pl.BlockSpec(memory_space=pltpu.VMEM)
SMEM = pl.BlockSpec(memory_space=pltpu.SMEM)
PARAMS = pltpu.CompilerParams(vmem_limit_bytes=48 * 1024 * 1024)


def attention(info, q, own, rest):
    rows, cols = q.shape
    group = cols // HEAD_DIM
    count = own.shape[0]
    return pl.pallas_call(
        attention_kernel,
        out_shape=jax.ShapeDtypeStruct((rows, cols), BF16),
        in_specs=[SMEM] + [VMEM] * (2 + len(rest)),
        out_specs=VMEM,
        scratch_shapes=[
            pltpu.VMEM((len(rest), *own.shape), BF16),
            pltpu.VMEM((group, 1, rows), F32),
            pltpu.VMEM((group, 1, rows), F32),
            pltpu.VMEM((group, HEAD_DIM, rows), F32),
            pltpu.VMEM((group, count, rows), F32),
            pltpu.VMEM((group, count, rows), BF16),
        ],
        compiler_params=PARAMS,
        name="causal_attention",
    )(info, q, own, *rest)


def projection_kernel(order, place_ref, vis_ref, *refs):
    pieces, w_ref, out_ref = refs[:-2], refs[-2], refs[-1]
    rows, width = pieces[0].shape[1:]
    total = None
    for j, piece in enumerate(pieces):
        for i in range(piece.shape[0]):
            head = order[j * piece.shape[0] + i]
            start = pl.multiple_of(head * width, width)
            both = jnp.concatenate([piece[i], vis_ref[head]], axis=0)
            part = jnp.dot(both, w_ref[pl.ds(start, width), :], preferred_element_type=F32)
            total = part if total is None else total + part
    placed = jnp.dot(place_ref[...], total[rows:].astype(BF16), preferred_element_type=F32)
    out_ref[...] = (total[:rows] + placed).astype(BF16)


def projection(order, placing, vis, pieces, weights, at, cols):
    rows = placing.shape[0]
    return pl.pallas_call(
        projection_kernel,
        grid=(1,),
        out_shape=jax.ShapeDtypeStruct((rows, cols), BF16),
        in_specs=[SMEM]
        + [VMEM] * (2 + len(pieces))
        + [pl.BlockSpec((weights.shape[0], cols), lambda i: (0, at))],
        out_specs=VMEM,
        compiler_params=PARAMS,
        name="decoder_projection",
    )(order, placing, vis, *pieces, weights)


def gathered_apart(value, axes):
    n, me = axis_len(axes), lax.axis_index(axes)
    done = jnp.zeros((n, *value.shape), value.dtype)
    for step in range(n):
        piece = value
        if step:
            piece = lax.ppermute(value, axes, [(i, i ^ step) for i in range(n)])
        done = lax.dynamic_update_index_in_dim(done, piece, me ^ step, 0)
    return done


def turned_if(value, flag, axis):
    return jnp.where(flag == 1, jnp.flip(value, axis), value)


def normed_tiles(tiles, gain, c, xl):
    heads, rows, cols = tiles.shape
    r = rows // 4
    wide = tiles.astype(F32).reshape(heads, 4, r, cols)
    count = heads * 4 * cols
    mean_sq = jnp.sum(wide * wide, axis=(0, 1, 3), keepdims=True) / count
    g = jnp.transpose(gain.reshape(4, heads, cols), (1, 0, 2))[:, :, None, :]
    normed = (wide * lax.rsqrt(mean_sq + 1e-06) * g).astype(BF16)
    zn = axis_len("z")
    split = normed.reshape(zn // 2, 2, 2, 2, r, cols)
    split = turned_if(turned_if(split, xl, 1), c, 2)
    return jnp.transpose(split, (3, 0, 2, 1, 4, 5)).reshape(zn, 4, r, cols)


def merger_kernel(got_ref, *refs, level):
    weights, out_ref = refs[:-1], refs[-1]
    zn, _, r, _ = got_ref.shape
    cols = weights[0].shape[1]
    total = None
    for i, w in enumerate(weights):
        rows = got_ref[:, i, :, :cols].reshape(zn * r, cols)
        part = jnp.dot(rows, w[level], preferred_element_type=F32)
        total = part if total is None else total + part
    out_ref[...] = total.astype(BF16).reshape(out_ref.shape)


def projected(got, weights, level):
    zn, _, r, _ = got.shape
    part = pl.pallas_call(
        functools.partial(merger_kernel, level=level),
        out_shape=jax.ShapeDtypeStruct((zn, r, weights[0].shape[2]), BF16),
        in_specs=[VMEM] * (1 + len(weights)),
        out_specs=VMEM,
        compiler_params=PARAMS,
        name="merger_product",
    )(got, *weights)
    back = exchange(part, "z")
    return back.astype(F32).sum(axis=0).astype(BF16)


def shards(
    patches, frames, enc_qkv, enc_out, merge_gain, merge_w, embedded, source, dec_q, dec_kv, cotangent
):
    place = lax.axis_index(PL)
    z, c, xl = lax.axis_index("z"), lax.axis_index("c"), lax.axis_index("xl")
    pat_rows, pat_cols = patches.shape
    tok_rows = embedded.shape[0]
    merged_rows = pat_rows // 4
    places = axis_len(PL)
    zn = axis_len("z")

    dec_w = lax.all_gather(jnp.concatenate([dec_q, dec_kv], axis=1), PL, axis=0, tiled=True)

    new = jnp.arange(pat_rows, dtype=jnp.int32)
    old = (new % merged_rows) * 4 + new // merged_rows
    reorder = (old[:, None] == jnp.arange(pat_rows, dtype=jnp.int32)[None, :]).astype(BF16)
    mine = dot(reorder, patches).astype(BF16)
    tiles = from_everyone(mine, HD)
    w_c = [merge_w] + [lax.ppermute(merge_w, ("c", "xl"), [(i, i ^ n) for i in range(4)]) for n in (1, 2, 3)]
    sources = gathered_apart(source, ("c", "xl")) + 1
    text = jnp.where((source >= 0)[:, None], BF16(0), embedded)
    text2, _ = lax.optimization_barrier((jnp.stack([text, swapped(text, "xh")]), tiles))
    yn = axis_len("y")
    pieces = [text2] + [
        lax.ppermute(text2, "y", [(i, i ^ n) for i in range(yn)]) for n in range(1, yn)
    ]
    xh, y = lax.axis_index("xh"), lax.axis_index("y")
    order = jnp.stack([(xh ^ i) * yn + (y ^ n) for n in range(yn) for i in range(2)]).astype(jnp.int32)

    coded = jnp.stack([sources // 64, sources % 64], axis=1).astype(BF16)
    coded = coded.reshape(4, merged_rows, -1)
    send = normed_tiles(tiles, merge_gain[0], c, xl)
    send = jnp.concatenate([send, jnp.broadcast_to(coded[None], (zn, *coded.shape))], axis=3)
    got, _ = lax.optimization_barrier((exchange(send, "z"), text2))
    merged0 = projected(got, w_c, 0)
    codes = got[..., pat_cols:].astype(jnp.int32).reshape(zn, 2, 2, 2, tok_rows)
    codes = codes[:, :, :, 0] * 64 + codes[:, :, :, 1] - 1
    all_source = jnp.transpose(codes, (1, 0, 2, 3)).reshape(places, tok_rows)

    row_ids = jnp.arange(tok_rows, dtype=jnp.int32)
    before = row_ids[:, None] < row_ids[None, :]
    wanted = (all_source >= 0) & (all_source // merged_rows == place)
    rank = dot(wanted.astype(BF16), before.astype(BF16)).astype(jnp.int32)
    rank = jnp.where(wanted, rank, -1)
    slot_ids = jnp.arange(RETURN_MOST, dtype=jnp.int32)
    local = jnp.sum(
        jnp.where(
            rank[:, None, :] == slot_ids[None, :, None], all_source[:, None, :] % merged_rows + 1, 0
        ),
        axis=2,
    ).reshape(-1) - 1
    merged_ids = jnp.arange(merged_rows, dtype=jnp.int32)
    setter = (merged_ids[:, None] == local[None, :]).astype(BF16)

    visual = source >= 0
    holder = jnp.where(visual, source // merged_rows, -1)
    earlier = (holder[:, None] == holder[None, :]) & before.T
    order_rank = jnp.sum(earlier.astype(jnp.int32), axis=1)
    bucket_slot = jnp.where(visual, holder * RETURN_MOST + order_rank, -1)
    slots = places * RETURN_MOST
    placer = jnp.arange(slots, dtype=jnp.int32)[:, None] == bucket_slot[None, :]
    vis_rank = jnp.sum((visual[None, :] & before.T).astype(jnp.int32), axis=1)
    chosen = visual[None, :] & (merged_ids[:, None] == vis_rank[None, :])
    slot_of = jnp.sum(jnp.where(chosen, bucket_slot[None, :] + 1, 0), axis=1) - 1
    fetch = (slot_of[:, None] == jnp.arange(slots, dtype=jnp.int32)[None, :]).astype(BF16)
    chosen_bf = chosen.astype(BF16)

    taken = exchange(dot(setter.T, merged0).astype(BF16), PL)
    vis_states = (dot(chosen_bf, embedded) + dot(fetch, taken)).astype(BF16)
    vis_states, _ = lax.optimization_barrier((vis_states, pieces))
    vis_tiles = from_everyone(vis_states, HD)

    placing = chosen_bf.T
    query_cols, pair_cols = dec_q.shape[1], dec_kv.shape[1]
    kv = projection(order, placing, vis_tiles, pieces, dec_w, query_cols // pair_cols, pair_cols)
    queries = projection(order, placing, vis_tiles, pieces, dec_w, 0, query_cols)

    pair = jnp.concatenate([kv, swapped(kv, "xl")], axis=0)
    up, down = [pair], [pair]
    near, away = [], []
    for step in range(1, zn // 2 + 1):
        up.append(shifted(up[-1], "z", 1))
        near.append(up[-1])
        away.append(-step)
        if step < zn // 2:
            down.append(shifted(down[-1], "z", -1))
            near.append(down[-1])
            away.append(step)
    far = [swapped(b, "c") for b in [pair] + near]
    seen = [((z + a) % zn < z).astype(jnp.int32) for a in away]
    info = jnp.stack([xl] + seen + [c] * len(far)).astype(jnp.int32)
    context = attention(info, queries, pair, near + far)

    full_patches = in_order(tiles)
    local_cols = enc_qkv.shape[2]
    enc_dim = full_patches.shape[1] // ENC_HEADS
    local_heads = local_cols // enc_dim
    enc_q = dot(full_patches, enc_qkv[0]).astype(BF16)
    enc_k = dot(full_patches, enc_qkv[1]).astype(BF16)
    enc_v = dot(full_patches, enc_qkv[2]).astype(BF16)
    paired = jnp.concatenate([enc_k, enc_v], axis=1)
    upward = [(i, i + 1) for i in range(places - 1)]
    low = lax.ppermute(paired, PL, upward)
    high = lax.ppermute(paired, PL, [(b, a) for a, b in upward])
    widened = jnp.concatenate([low, paired, high], axis=0)
    padded = jnp.pad(frames, (pat_rows, pat_rows), constant_values=-1)
    key_frames = lax.dynamic_slice_in_dim(padded, place * pat_rows, 3 * pat_rows)
    key_frames = jnp.swapaxes(key_frames.reshape(3, merged_rows, 4), 1, 2).reshape(-1)
    own_frames = key_frames[pat_rows : 2 * pat_rows]
    same = own_frames[:, None] == key_frames[None, :]
    query3 = enc_q.reshape(pat_rows, local_heads, enc_dim)
    keys3 = widened[:, :local_cols].reshape(3 * pat_rows, local_heads, enc_dim)
    values3 = widened[:, local_cols:].reshape(3 * pat_rows, local_heads, enc_dim)
    scores = jnp.einsum("qhd,khd->hqk", query3, keys3, preferred_element_type=F32) / jnp.sqrt(
        F32(enc_dim)
    )
    scores = jnp.where(same[None], scores, F32(-1e30))
    top = jnp.max(scores, axis=2, keepdims=True)
    weights = jnp.where(same[None], jnp.exp(scores - top), F32(0.0))
    total = jnp.sum(weights, axis=2)
    mixed = jnp.einsum("hqk,khd->qhd", weights.astype(BF16), values3, preferred_element_type=F32)
    enc_attn = (
        (mixed / jnp.transpose(total)[:, :, None]).astype(BF16).reshape(pat_rows, local_cols)
    )
    enc_attn, _ = lax.optimization_barrier((enc_attn, vis_tiles))
    partial_out = dot(enc_attn, enc_out).astype(BF16)
    outs = jnp.moveaxis(partial_out.reshape(pat_rows, axis_len(HD), local_cols), 1, 0)
    summed = exchange(outs, HD).astype(F32).sum(axis=0)
    enc_hidden = (mine.astype(F32) + summed).astype(BF16)
    send1 = normed_tiles(from_everyone(enc_hidden, HD), merge_gain[1], c, xl)
    send1, _ = lax.optimization_barrier((send1, (up[1], down[1])))
    got1 = exchange(send1, "z")
    merged1 = projected(got1, w_c, 1)

    cot_flat = cotangent.reshape(tok_rows, 2 * cotangent.shape[2])
    bucket_rows = dot(placer.astype(BF16), cot_flat).astype(BF16)
    bucket_rows, _ = lax.optimization_barrier((bucket_rows, merged1))
    arrived_rows = exchange(bucket_rows, PL)
    returned = dot(setter, arrived_rows)
    level_grads = jnp.transpose(returned.reshape(merged_rows, 2, cotangent.shape[2]), (1, 0, 2))
    return jnp.stack([merged0, merged1]), context, level_grads


def solution(mesh):
    fine = Mesh(mesh.devices.reshape(2, 8, 2, 2, 4), ("c", "z", "xl", "xh", "y"))
    in_specs = (
        P(PL, HD),
        P(),
        P(None, None, HD),
        P(HD, None),
        P(),
        P(None, PL, HD),
        P(PL, HD),
        P(PL),
        P(PL, HD),
        P(PL, HD),
        P(PL, None, HD),
    )
    out_specs = (P(None, PL, HD), P(PL, HD), P(None, PL, HD))
    return jax.shard_map(shards, mesh=fine, in_specs=in_specs, out_specs=out_specs, check_vma=False)
```

```python
import functools

import jax
import jax.numpy as jnp
from jax import lax
from jax.experimental import pallas as pl
from jax.experimental.pallas import tpu as pltpu
from jax.sharding import Mesh, PartitionSpec as P

ENC_HEADS = 16
HEAD_DIM = 128
RETURN_MOST = 4
PL = ("c", "z", "xl")
HD = ("xh", "y")
F32 = jnp.float32
BF16 = jnp.bfloat16


def axis_len(axes):
    return lax.axis_size(axes)


def exchange(tiles, axes):
    return lax.all_to_all(tiles, axes, 0, 0, tiled=True)


def from_everyone(value, axes):
    return exchange(jnp.broadcast_to(value[None], (axis_len(axes), *value.shape)), axes)


def in_order(tiles):
    return jnp.moveaxis(tiles, 0, 1).reshape(tiles.shape[1], -1)


def swapped(value, axis):
    return lax.ppermute(value, axis, [(0, 1), (1, 0)])


def shifted(value, axis, by):
    n = axis_len(axis)
    return lax.ppermute(value, axis, [(i, (i + by) % n) for i in range(n)])


def dot(a, b):
    return jnp.dot(a, b, preferred_element_type=F32)


FACTOR = 1.4426950408889634 / HEAD_DIM**0.5
CHUNK = 64


def take_block(heads, q_ref, block, mask, m_ref, l_ref, acc_ref, s_ref, p_ref):
    keys, values = block[:, :HEAD_DIM], block[:, HEAD_DIM:]
    count, rows = keys.shape[0], q_ref.shape[0]
    first = mask is not None
    turned = values.T
    for h in heads:
        q = q_ref[:, pl.ds(pl.multiple_of(h * HEAD_DIM, HEAD_DIM), HEAD_DIM)]
        s_ref[h] = lax.dot_general(keys, q, (((1,), (1,)), ((), ())), preferred_element_type=F32)
    for h in heads:
        top = None
        for i in range(0, count, CHUNK):
            s = s_ref[h, i : i + CHUNK]
            if first:
                s = jnp.where(mask(i), s, F32(-1e30))
                s_ref[h, i : i + CHUNK] = s
            t = jnp.max(s.reshape(CHUNK // 8, 8, rows), axis=0)
            top = t if top is None else jnp.maximum(top, t)
        top = jnp.max(top, axis=0, keepdims=True)
        if not first:
            top = jnp.maximum(m_ref[h], top)
        total = None
        for i in range(0, count, CHUNK):
            p = jnp.exp2((s_ref[h, i : i + CHUNK] - top) * F32(FACTOR))
            t = jnp.sum(p.reshape(CHUNK // 8, 8, rows), axis=0)
            total = t if total is None else total + t
            p_ref[h, i : i + CHUNK] = p.astype(BF16)
        total = jnp.sum(total, axis=0, keepdims=True)
        mixed = jnp.dot(turned, p_ref[h], preferred_element_type=F32)
        if not first:
            keep = jnp.exp2((m_ref[h] - top) * F32(FACTOR))
            total = total + l_ref[h] * keep
            mixed = mixed + acc_ref[h] * keep
        m_ref[h], l_ref[h], acc_ref[h] = top, total, mixed


def attention_kernel(info, q_ref, own_ref, *refs):
    rest, out_ref, buffer, scratch = refs[:-7], refs[-7], refs[-6], refs[-5:]
    rows = q_ref.shape[0]
    group = q_ref.shape[1] // HEAD_DIM
    limit = jnp.where(info[0] == 1, 2 * rows, 0)

    def mask(start):
        key = lax.broadcasted_iota(jnp.int32, (CHUNK, rows), 0) + start
        query = lax.broadcasted_iota(jnp.int32, (CHUNK, rows), 1)
        return (key <= query) | ((key >= rows) & (key < limit))

    for i, ref in enumerate(rest):
        buffer[i] = ref[...]
    def own_step(h, _):
        take_block([h], q_ref, own_ref[...], mask, *scratch)
        return 0

    lax.fori_loop(0, group, own_step, 0)

    def step(i, _):
        @pl.when(info[1 + i] == 1)
        def _():
            take_block(range(group), q_ref, buffer[i], None, *scratch)

        return 0

    lax.fori_loop(0, len(rest), step, 0)

    acc_ref, l_ref = scratch[2], scratch[1]
    for h in range(group):
        out = acc_ref[h] / l_ref[h]
        out_ref[:, h * HEAD_DIM : (h + 1) * HEAD_DIM] = out.T.astype(BF16)


VMEM = pl.BlockSpec(memory_space=pltpu.VMEM)
SMEM = pl.BlockSpec(memory_space=pltpu.SMEM)
PARAMS = pltpu.CompilerParams(vmem_limit_bytes=48 * 1024 * 1024)


def attention(info, q, own, rest):
    rows, cols = q.shape
    group = cols // HEAD_DIM
    count = own.shape[0]
    return pl.pallas_call(
        attention_kernel,
        out_shape=jax.ShapeDtypeStruct((rows, cols), BF16),
        in_specs=[SMEM] + [VMEM] * (2 + len(rest)),
        out_specs=VMEM,
        scratch_shapes=[
            pltpu.VMEM((len(rest), *own.shape), BF16),
            pltpu.VMEM((group, 1, rows), F32),
            pltpu.VMEM((group, 1, rows), F32),
            pltpu.VMEM((group, HEAD_DIM, rows), F32),
            pltpu.VMEM((group, count, rows), F32),
            pltpu.VMEM((group, count, rows), BF16),
        ],
        compiler_params=PARAMS,
        name="causal_attention",
    )(info, q, own, *rest)


def projection_kernel(order, place_ref, vis_ref, *refs):
    pieces, w_ref, out_ref = refs[:-2], refs[-2], refs[-1]
    rows, width = pieces[0].shape[1:]
    total = None
    for j, piece in enumerate(pieces):
        for i in range(piece.shape[0]):
            head = order[j * piece.shape[0] + i]
            start = pl.multiple_of(head * width, width)
            both = jnp.concatenate([piece[i], vis_ref[head]], axis=0)
            part = jnp.dot(both, w_ref[pl.ds(start, width), :], preferred_element_type=F32)
            total = part if total is None else total + part
    placed = jnp.dot(place_ref[...], total[rows:].astype(BF16), preferred_element_type=F32)
    out_ref[...] = (total[:rows] + placed).astype(BF16)


def projection(order, placing, vis, pieces, weights, at, cols):
    rows = placing.shape[0]
    return pl.pallas_call(
        projection_kernel,
        grid=(1,),
        out_shape=jax.ShapeDtypeStruct((rows, cols), BF16),
        in_specs=[SMEM]
        + [VMEM] * (2 + len(pieces))
        + [pl.BlockSpec((weights.shape[0], cols), lambda i: (0, at))],
        out_specs=VMEM,
        compiler_params=PARAMS,
        name="decoder_projection",
    )(order, placing, vis, *pieces, weights)


def gathered_apart(value, axes):
    n, me = axis_len(axes), lax.axis_index(axes)
    done = jnp.zeros((n, *value.shape), value.dtype)
    for step in range(n):
        piece = value
        if step:
            piece = lax.ppermute(value, axes, [(i, i ^ step) for i in range(n)])
        done = lax.dynamic_update_index_in_dim(done, piece, me ^ step, 0)
    return done


def turned_if(value, flag, axis):
    return jnp.where(flag == 1, jnp.flip(value, axis), value)


def normed_tiles(tiles, gain, c, xl):
    heads, rows, cols = tiles.shape
    r = rows // 4
    wide = tiles.astype(F32).reshape(heads, 4, r, cols)
    count = heads * 4 * cols
    mean_sq = jnp.sum(wide * wide, axis=(0, 1, 3), keepdims=True) / count
    g = jnp.transpose(gain.reshape(4, heads, cols), (1, 0, 2))[:, :, None, :]
    normed = (wide * lax.rsqrt(mean_sq + 1e-06) * g).astype(BF16)
    zn = axis_len("z")
    split = normed.reshape(zn // 2, 2, 2, 2, r, cols)
    split = turned_if(turned_if(split, xl, 1), c, 2)
    return jnp.transpose(split, (3, 0, 2, 1, 4, 5)).reshape(zn, 4, r, cols)


def merger_kernel(got_ref, *refs, level):
    weights, out_ref = refs[:-1], refs[-1]
    zn, _, r, _ = got_ref.shape
    cols = weights[0].shape[1]
    total = None
    for i, w in enumerate(weights):
        rows = got_ref[:, i, :, :cols].reshape(zn * r, cols)
        part = jnp.dot(rows, w[level], preferred_element_type=F32)
        total = part if total is None else total + part
    out_ref[...] = total.astype(BF16).reshape(out_ref.shape)


def merger_part(got, weights, level):
    zn, _, r, _ = got.shape
    return pl.pallas_call(
        functools.partial(merger_kernel, level=level),
        out_shape=jax.ShapeDtypeStruct((zn, r, weights[0].shape[2]), BF16),
        in_specs=[VMEM] * (1 + len(weights)),
        out_specs=VMEM,
        compiler_params=PARAMS,
        name="merger_product",
    )(got, *weights)


def merger_sum(part):
    back = exchange(part, "z")
    return back.astype(F32).sum(axis=0).astype(BF16)


def shards(
    patches, frames, enc_qkv, enc_out, merge_gain, merge_w, embedded, source, dec_q, dec_kv, cotangent
):
    place = lax.axis_index(PL)
    z, c, xl = lax.axis_index("z"), lax.axis_index("c"), lax.axis_index("xl")
    pat_rows, pat_cols = patches.shape
    tok_rows = embedded.shape[0]
    merged_rows = pat_rows // 4
    places = axis_len(PL)
    zn = axis_len("z")

    dec_w = lax.all_gather(jnp.concatenate([dec_q, dec_kv], axis=1), PL, axis=0, tiled=True)

    new = jnp.arange(pat_rows, dtype=jnp.int32)
    old = (new % merged_rows) * 4 + new // merged_rows
    reorder = (old[:, None] == jnp.arange(pat_rows, dtype=jnp.int32)[None, :]).astype(BF16)
    mine = dot(reorder, patches).astype(BF16)
    tiles = from_everyone(mine, HD)
    text = jnp.where((source >= 0)[:, None], BF16(0), embedded)
    merge_late, text, _ = lax.optimization_barrier((merge_w, text, tiles))
    w_c = [merge_w] + [lax.ppermute(merge_late, ("c", "xl"), [(i, i ^ n) for i in range(4)]) for n in (1, 2, 3)]
    text2 = jnp.stack([text, swapped(text, "xh")])
    yn = axis_len("y")
    pieces = [text2] + [
        lax.ppermute(text2, "y", [(i, i ^ n) for i in range(yn)]) for n in range(1, yn)
    ]
    xh, y = lax.axis_index("xh"), lax.axis_index("y")
    order = jnp.stack([(xh ^ i) * yn + (y ^ n) for n in range(yn) for i in range(2)]).astype(jnp.int32)

    coded = jnp.stack([(source + 1) // 64, (source + 1) % 64]).astype(BF16)
    coded = coded.reshape(merged_rows, -1)
    send = normed_tiles(tiles, merge_gain[0], c, xl)
    send = jnp.concatenate([send, jnp.broadcast_to(coded, (zn, 4, *coded.shape))], axis=3)
    got, _ = lax.optimization_barrier((exchange(send, "z"), text2))
    part0 = merger_part(got, w_c, 0)
    merged0 = merger_sum(part0)
    codes, _ = lax.optimization_barrier((got[:, 0, :, pat_cols:], part0))
    codes = codes.astype(jnp.int32).reshape(zn, 2, tok_rows)
    codes = gathered_apart(codes[:, 0] * 64 + codes[:, 1] - 1, ("c", "xl"))
    codes = codes.reshape(2, 2, zn, tok_rows)
    all_source = jnp.transpose(codes, (0, 2, 1, 3)).reshape(places, tok_rows)

    row_ids = jnp.arange(tok_rows, dtype=jnp.int32)
    before = row_ids[:, None] < row_ids[None, :]
    wanted = (all_source >= 0) & (all_source // merged_rows == place)
    rank = dot(wanted.astype(BF16), before.astype(BF16)).astype(jnp.int32)
    rank = jnp.where(wanted, rank, -1)
    slot_ids = jnp.arange(RETURN_MOST, dtype=jnp.int32)
    local = jnp.sum(
        jnp.where(
            rank[:, None, :] == slot_ids[None, :, None], all_source[:, None, :] % merged_rows + 1, 0
        ),
        axis=2,
    ).reshape(-1) - 1
    merged_ids = jnp.arange(merged_rows, dtype=jnp.int32)
    setter = (merged_ids[:, None] == local[None, :]).astype(BF16)

    visual = source >= 0
    holder = jnp.where(visual, source // merged_rows, -1)
    earlier = (holder[:, None] == holder[None, :]) & before.T
    order_rank = jnp.sum(earlier.astype(jnp.int32), axis=1)
    bucket_slot = jnp.where(visual, holder * RETURN_MOST + order_rank, -1)
    slots = places * RETURN_MOST
    placer = jnp.arange(slots, dtype=jnp.int32)[:, None] == bucket_slot[None, :]
    vis_rank = jnp.sum((visual[None, :] & before.T).astype(jnp.int32), axis=1)
    chosen = visual[None, :] & (merged_ids[:, None] == vis_rank[None, :])
    slot_of = jnp.sum(jnp.where(chosen, bucket_slot[None, :] + 1, 0), axis=1) - 1
    fetch = (slot_of[:, None] == jnp.arange(slots, dtype=jnp.int32)[None, :]).astype(BF16)
    chosen_bf = chosen.astype(BF16)

    taken = exchange(dot(setter.T, merged0).astype(BF16), PL)
    vis_states = (dot(chosen_bf, embedded) + dot(fetch, taken)).astype(BF16)
    vis_states, _ = lax.optimization_barrier((vis_states, pieces))
    vis_tiles = from_everyone(vis_states, HD)

    placing = chosen_bf.T
    query_cols, pair_cols = dec_q.shape[1], dec_kv.shape[1]
    kv = projection(order, placing, vis_tiles, pieces, dec_w, query_cols // pair_cols, pair_cols)
    queries = projection(order, placing, vis_tiles, pieces, dec_w, 0, query_cols)

    pair = jnp.concatenate([kv, swapped(kv, "xl")], axis=0)
    up, down = [pair], [pair]
    near, away = [], []
    for step in range(1, zn // 2 + 1):
        if step == 2:
            up[1], down[1], queries = lax.optimization_barrier((up[1], down[1], queries))
        up.append(shifted(up[-1], "z", 1))
        near.append(up[-1])
        away.append(-step)
        if step < zn // 2:
            down.append(shifted(down[-1], "z", -1))
            near.append(down[-1])
            away.append(step)
    far = [swapped(b, "c") for b in [pair] + near]
    seen = [((z + a) % zn < z).astype(jnp.int32) for a in away]
    info = jnp.stack([xl] + seen + [c] * len(far)).astype(jnp.int32)
    context = attention(info, queries, pair, near + far)

    full_patches = in_order(tiles)
    local_cols = enc_qkv.shape[2]
    enc_dim = full_patches.shape[1] // ENC_HEADS
    local_heads = local_cols // enc_dim
    enc_q = dot(full_patches, enc_qkv[0]).astype(BF16)
    enc_k = dot(full_patches, enc_qkv[1]).astype(BF16)
    enc_v = dot(full_patches, enc_qkv[2]).astype(BF16)
    paired = jnp.concatenate([enc_k, enc_v], axis=1)
    upward = [(i, i + 1) for i in range(places - 1)]
    low = lax.ppermute(paired, PL, upward)
    high = lax.ppermute(paired, PL, [(b, a) for a, b in upward])
    widened = jnp.concatenate([low, paired, high], axis=0)
    padded = jnp.pad(frames, (pat_rows, pat_rows), constant_values=-1)
    key_frames = lax.dynamic_slice_in_dim(padded, place * pat_rows, 3 * pat_rows)
    key_frames = jnp.swapaxes(key_frames.reshape(3, merged_rows, 4), 1, 2).reshape(-1)
    own_frames = key_frames[pat_rows : 2 * pat_rows]
    same = own_frames[:, None] == key_frames[None, :]
    query3 = enc_q.reshape(pat_rows, local_heads, enc_dim)
    keys3 = widened[:, :local_cols].reshape(3 * pat_rows, local_heads, enc_dim)
    values3 = widened[:, local_cols:].reshape(3 * pat_rows, local_heads, enc_dim)
    scores = jnp.einsum("qhd,khd->hqk", query3, keys3, preferred_element_type=F32) / jnp.sqrt(
        F32(enc_dim)
    )
    scores = jnp.where(same[None], scores, F32(-1e30))
    top = jnp.max(scores, axis=2, keepdims=True)
    weights = jnp.where(same[None], jnp.exp(scores - top), F32(0.0))
    total = jnp.sum(weights, axis=2)
    mixed = jnp.einsum("hqk,khd->qhd", weights.astype(BF16), values3, preferred_element_type=F32)
    enc_attn = (
        (mixed / jnp.transpose(total)[:, :, None]).astype(BF16).reshape(pat_rows, local_cols)
    )
    partial_out = dot(enc_attn, enc_out)
    outs = jnp.moveaxis(partial_out.reshape(pat_rows, 2, yn, local_cols), 0, 2)
    kept = lax.dynamic_index_in_dim(outs, xh, 0, False)
    sent = lax.dynamic_index_in_dim(outs, 1 - xh, 0, False).astype(BF16)
    half = kept + swapped(sent, "xh").astype(F32)
    summed = lax.dynamic_index_in_dim(half, y, 0, False)
    for n in range(1, yn):
        sent = lax.dynamic_index_in_dim(half, y ^ n, 0, False).astype(BF16)
        summed = summed + lax.ppermute(sent, "y", [(i, i ^ n) for i in range(yn)]).astype(F32)
    enc_hidden = (mine.astype(F32) + summed).astype(BF16)
    mine_half = gathered_apart(enc_hidden, "y")
    other_half = swapped(mine_half, "xh")
    hidden_tiles = jnp.concatenate(
        [jnp.where(xh == 0, mine_half, other_half), jnp.where(xh == 0, other_half, mine_half)]
    )

    cot_flat = cotangent.reshape(tok_rows, 2 * cotangent.shape[2])
    bucket_rows = dot(placer.astype(BF16), cot_flat).astype(BF16)
    bucket_rows, _ = lax.optimization_barrier((bucket_rows, kv))
    arrived_rows = exchange(bucket_rows, PL)

    send1 = normed_tiles(hidden_tiles, merge_gain[1], c, xl)
    send1, _ = lax.optimization_barrier((send1, (arrived_rows, up[1], down[1])))
    part1 = merger_part(exchange(send1, "z"), w_c, 1)
    part1, _ = lax.optimization_barrier((part1, far))
    merged1 = merger_sum(part1)

    returned = dot(setter, arrived_rows)
    level_grads = jnp.transpose(returned.reshape(merged_rows, 2, cotangent.shape[2]), (1, 0, 2))
    return jnp.stack([merged0, merged1]), context, level_grads


def solution(mesh):
    fine = Mesh(mesh.devices.reshape(2, 8, 2, 2, 4), ("c", "z", "xl", "xh", "y"))
    in_specs = (
        P(PL, HD),
        P(),
        P(None, None, HD),
        P(HD, None),
        P(),
        P(None, PL, HD),
        P(PL, HD),
        P(PL),
        P(PL, HD),
        P(PL, HD),
        P(PL, None, HD),
    )
    out_specs = (P(None, PL, HD), P(PL, HD), P(None, PL, HD))
    return jax.shard_map(shards, mesh=fine, in_specs=in_specs, out_specs=out_specs, check_vma=False)
```
